32 devices in a mesh: dp: 4 (over y, x), fsdp: 8 (over z, core).
Axes of the slice: x: 2, y: 2, z: 4, core: 2. Of those that a mesh axis runs over, the one named last changes fastest.
Arguments:
- hidden: bfloat16 [16384, 4096], P(('dp', 'fsdp')), may hold values from -6 to 6
- queries: bfloat16 [16384, 2048], P(('dp', 'fsdp')), may hold values from -60 to 60
- cotangent: bfloat16 [16384, 2048], P(('dp', 'fsdp')), may hold values from -0.125 to 0.125
- point_start: bfloat16 [4096, 1024], P('fsdp', 'dp'), may hold values from -0.09375 to 0.09375
- point_mid: bfloat16 [4096, 1024], P('fsdp', 'dp'), may hold values from -0.09375 to 0.09375
- point_end: bfloat16 [4096, 1024], P('fsdp', 'dp'), may hold values from -0.09375 to 0.09375
- curve_time: float32 [1], replicated, may hold values from 0.15 to 0.85
Outputs:
- context: bfloat16 [16384, 2048], P(('dp', 'fsdp'))
- gradient: float32 [4096, 1024], P('fsdp', 'dp')
The draws below stay inside these ranges and needn't reach their ends.
All inputs are finite; a program needn't handle non-finite values.
Results may differ from the reference program's by a relative error of at most 0.0071.
Values may be sent and summed in bfloat16 or wider, within the bound.
No kernel may reach another device: no remote copies, remote signals or barrier semaphores. Data moves between devices by JAX's collectives and lax.ppermute only.
A program may use at most 128 MiB of HBM per device.

```python
import math
import jax
import jax.numpy as jnp
from jax import lax

D = 4096
HQ = 16
KVH = 4
HD = 128
SEQ = 512
KVW = 512
TOKENS = 16384


def draw_queries(key, part):
    first_key = jax.random.fold_in(key, 0)
    base_draw = jnp.clip(jax.random.normal(first_key, (TOKENS, HQ * HD), jnp.float32), -4.0, 4.0)
    return base_draw.astype(jnp.bfloat16)


def spiked(drawn, own_key, source, target, blocks, factor):
    owner, partner = [(jnp.arange(drawn.shape[position]) // (drawn.shape[position] // blocks)).reshape([-1 if axis == position else 1 for axis in range(drawn.ndim)]) for position in (source, target)]
    chosen = jax.random.permutation(own_key, blocks)[partner]
    strong = (owner == chosen) | (owner == (partner + blocks // 2) % blocks)
    return jnp.where(strong, factor * drawn, drawn)


def levels(stream_key, extent, cuts, least, top_value):
    gain = 1.0
    for axis_at, parts in cuts:
        steps = jax.random.uniform(jax.random.fold_in(jax.random.fold_in(stream_key, 6), axis_at), (parts,), jnp.float32, least / len(cuts), top_value / len(cuts))
        gain = gain * jnp.repeat(jnp.exp(steps), extent[axis_at] // parts).reshape((-1,) + (1,) * (len(extent) - 1 - axis_at))
    return gain


def centred(own_key, dims, scale, limit, cuts=(), held_as=jnp.bfloat16):
    entries = scale * jax.random.normal(own_key, dims, jnp.float32)
    if cuts:
        entries = entries * levels(own_key, dims, cuts, -0.22, 0.18)
    return jnp.clip(entries, -limit, limit).astype(held_as)


def heavy_noise(own_key, extent, scale, reach, cuts, heavy, held_as=jnp.bfloat16):
    values = scale * jax.random.normal(own_key, extent, jnp.float32)
    if cuts:
        values = values * levels(own_key, extent, cuts, -0.22, 0.18)
    return jnp.clip(spiked(values, jax.random.fold_in(own_key, 3), *heavy), -reach, reach).astype(held_as)


def setup_inputs(seed: int = 0) -> dict:
    splits = jax.random.split(jax.random.key(seed), 8)
    return {
        "hidden": heavy_noise(splits[0], (TOKENS, D), 1.0, 6.0, ((0, 32),), (0, 1, 32, 2.75)),
        "queries": draw_queries(jax.random.fold_in(splits[7], 71), 0),
        "cotangent": centred(splits[2], (TOKENS, HQ * HD), (TOKENS ** -0.5), 0.125, ((0, 32),)),
        "point_start": centred(splits[3], (D, 2 * KVW), D ** -0.5, 0.09375, ((0, 8), (1, 4))),
        "point_mid": centred(splits[4], (D, 2 * KVW), D ** -0.5, 0.09375, ((0, 8), (1, 4))),
        "point_end": centred(splits[5], (D, 2 * KVW), D ** -0.5, 0.09375, ((0, 8), (1, 4))),
        "curve_time": jnp.clip(jax.random.uniform(splits[6], (1,), jnp.float32, 0.15, 0.85), 0.15, 0.85),
    }


def rope_tables(seq_len, head_dim):
    positions = jnp.arange(seq_len, dtype=jnp.float32)[:, None]
    halves_index = jnp.arange(head_dim // 2, dtype=jnp.float32)[None, :]
    inverse = jnp.exp(-(2.0 * halves_index / head_dim) * math.log(500000.0))
    angles = positions * inverse
    cosine = jnp.concatenate([jnp.cos(angles), jnp.cos(angles)], axis=1)
    sine_t = jnp.concatenate([jnp.sin(angles), jnp.sin(angles)], axis=1)
    return (cosine, sine_t)

def rotate(values_in):
    half_size = values_in.shape[-1] // 2
    return jnp.concatenate([-values_in[..., half_size:], values_in[..., :half_size]], axis=-1)

def rotate_back(values_in):
    half_size = values_in.shape[-1] // 2
    return jnp.concatenate([values_in[..., half_size:], -values_in[..., :half_size]], axis=-1)

def attend(kv_rows, query_rows, grad_rows, kv_heads, head_dim):
    seq_len = kv_rows.shape[0]
    kv_width = kv_heads * head_dim
    group_size = query_rows.shape[1] // kv_width
    width_head = group_size * head_dim
    cosine, sine_t = rope_tables(seq_len, head_dim)
    causal = jnp.arange(seq_len)[:, None] >= jnp.arange(seq_len)[None, :]
    score_scale = 1.0 / math.sqrt(head_dim)
    contexts = []
    key_grads = []
    value_grads = []
    for kv_head in range(kv_heads):
        keys_raw = kv_rows[:, kv_head * head_dim:(kv_head + 1) * head_dim].astype(jnp.float32)
        values_head = kv_rows[:, kv_width + kv_head * head_dim:kv_width + (kv_head + 1) * head_dim].astype(jnp.float32)
        keys_head = (keys_raw * cosine + rotate(keys_raw) * sine_t).astype(jnp.bfloat16).astype(jnp.float32)
        query_head = query_rows[:, kv_head * width_head:(kv_head + 1) * width_head].reshape(seq_len, group_size, head_dim).astype(jnp.float32)
        grad_head = grad_rows[:, kv_head * width_head:(kv_head + 1) * width_head].reshape(seq_len, group_size, head_dim).astype(jnp.float32)
        scores = jnp.einsum('sgd,td->gst', query_head, keys_head) * score_scale
        scores = jnp.where(causal[None], scores, -1e+30)
        top_score = lax.optimization_barrier(jnp.max(scores, axis=-1, keepdims=True))
        weights_exp = jnp.exp(scores - top_score)
        probs = weights_exp / lax.optimization_barrier(jnp.sum(weights_exp, axis=-1, keepdims=True))
        probs_low = probs.astype(jnp.bfloat16).astype(jnp.float32)
        context_head = jnp.einsum('gst,td->sgd', probs_low, values_head).astype(jnp.bfloat16)
        contexts.append(context_head.reshape(seq_len, width_head))
        prob_grad = jnp.einsum('sgd,td->gst', grad_head, values_head)
        value_grads.append(jnp.einsum('gst,sgd->td', probs_low, grad_head))
        score_grad = probs * (prob_grad - lax.optimization_barrier(jnp.sum(prob_grad * probs, axis=-1, keepdims=True))) * score_scale
        score_low = score_grad.astype(jnp.bfloat16).astype(jnp.float32)
        rot_grad = jnp.einsum('gst,sgd->td', score_low, query_head)
        key_grads.append(rot_grad * cosine + rotate_back(rot_grad * sine_t))
    context_rows = jnp.concatenate(contexts, axis=1)
    kv_grad = jnp.concatenate(key_grads + value_grads, axis=1).astype(jnp.bfloat16)
    return (context_rows, kv_grad)

def reference(hidden, queries, cotangent, point_start, point_mid, point_end, curve_time):
    t_value = curve_time[0]
    blended = ((1.0 - t_value) ** 2 * point_start.astype(jnp.float32) + 2.0 * t_value * (1.0 - t_value) * point_mid.astype(jnp.float32) + t_value ** 2 * point_end.astype(jnp.float32)).astype(jnp.bfloat16)
    kv_rows = jnp.dot(hidden, blended, preferred_element_type=jnp.float32).astype(jnp.bfloat16)
    seq_count = hidden.shape[0] // SEQ

    def one_sequence(items):
        return attend(items[0], items[1], items[2], KVH, HD)
    context_all, grad_all = lax.map(one_sequence, (kv_rows.reshape(seq_count, SEQ, -1), queries.reshape(seq_count, SEQ, -1), cotangent.reshape(seq_count, SEQ, -1)))
    context = context_all.reshape(hidden.shape[0], -1)
    kv_grad = grad_all.reshape(hidden.shape[0], -1)
    gradient = jnp.dot(hidden.T, kv_grad, preferred_element_type=jnp.float32) * (2.0 * t_value * (1.0 - t_value))
    return (context, gradient)
```

```python
import functools
import math

import jax
import jax.numpy as jnp
from jax import lax
from jax.experimental import pallas as pl
from jax.experimental.pallas import tpu as pltpu
from jax.sharding import PartitionSpec as P

KVH = 4
HD = 128
AXES = ("dp", "fsdp")


def rope_tables(seq_len, head_dim):
    positions = jnp.arange(seq_len, dtype=jnp.float32)[:, None]
    halves_index = jnp.arange(head_dim // 2, dtype=jnp.float32)[None, :]
    inverse = jnp.exp(-(2.0 * halves_index / head_dim) * math.log(500000.0))
    angles = positions * inverse
    cosine = jnp.concatenate([jnp.cos(angles), jnp.cos(angles)], axis=1)
    sine_t = jnp.concatenate([jnp.sin(angles), jnp.sin(angles)], axis=1)
    return (cosine, sine_t)


def swap(value, mask):
    count = lax.axis_size("dp") * lax.axis_size("fsdp")
    return lax.ppermute(value, AXES, [(i, i ^ mask) for i in range(count)])


def project_kernel(layout, has_sum, index_ref, hidden_ref, *rest):
    del index_ref
    refs, sum_ref, out_ref, acc_ref = rest[:-3], rest[-3], rest[-2], rest[-1]
    step = pl.program_id(0)
    blocks = []
    for part in layout:
        blocks.append(jnp.concatenate([refs[at][...] for at in part], axis=1))
    product = jnp.dot(
        hidden_ref[...], jnp.concatenate(blocks, axis=0), preferred_element_type=jnp.float32
    )

    @pl.when(step == 0)
    def _():
        acc_ref[...] = product + sum_ref[...] if has_sum else product

    @pl.when(step > 0)
    def _():
        acc_ref[...] += product

    @pl.when(step == pl.num_programs(0) - 1)
    def _():
        out_ref[...] = acc_ref[...].astype(out_ref.dtype)


def project(hidden, index, parts, rows, total, dtype):
    seq_len = hidden.shape[0]
    n_z = index.shape[0]
    span = rows // len(parts)
    flat, layout = [], []
    for part in parts:
        layout.append(list(range(len(flat), len(flat) + len(part))))
        flat.extend(part)
    width = HD * len(parts[0])
    whole = pl.BlockSpec((seq_len, width), lambda i, at: (0, 0))
    has_sum = total is not None
    if total is None:
        total = jnp.zeros((8, HD), jnp.float32)
    sum_spec = whole if has_sum else pl.BlockSpec((8, HD), lambda i, at: (0, 0))
    specs = [pl.BlockSpec((span, HD), lambda i, at, c=c: (i, c)) for _, c in flat]
    return pl.pallas_call(
        functools.partial(project_kernel, layout, has_sum),
        grid_spec=pltpu.PrefetchScalarGridSpec(
            num_scalar_prefetch=1,
            grid=(n_z,),
            in_specs=[pl.BlockSpec((seq_len, rows), lambda i, at: (0, at[i]))] + specs + [sum_spec],
            out_specs=whole,
            scratch_shapes=[pltpu.VMEM((seq_len, width), jnp.float32)],
        ),
        out_shape=jax.ShapeDtypeStruct((seq_len, width), dtype),
        cost_estimate=pl.CostEstimate(
            flops=8 * seq_len * n_z * rows * width,
            bytes_accessed=2 * n_z * rows * (seq_len + width),
            transcendentals=0,
        ),
        name="project",
    )(index, hidden, *[array for array, _ in flat], total)


def spread_kernel(n_dp, n_parts, sides, has_add, index_ref, hidden_ref, *rest):
    grads, rest = rest[:n_dp], rest[n_dp:]
    adds, outs, relative_ref = rest[: len(rest) - 1 - n_parts * len(sides[0])], None, rest[-1]
    outs = rest[len(adds) : -1]
    step = pl.program_id(0)

    @pl.when(step == 0)
    def _():
        me = index_ref[index_ref.shape[0] - 1]
        for k in range(n_dp):
            to = pl.multiple_of((k ^ me) * HD, HD)
            relative_ref[:, pl.ds(to, HD)] = grads[k][...]

    product = lax.dot_general(
        hidden_ref[...],
        relative_ref[...],
        (((0,), (0,)), ((), ())),
        preferred_element_type=jnp.float32,
    )
    span = product.shape[0] // n_parts
    for p in range(n_parts):
        share = product[p * span : (p + 1) * span]
        if has_add:
            share = share + adds[p][...].astype(jnp.float32)
        for side, columns in enumerate(sides[p]):
            out = outs[p * len(sides[p]) + side]
            for at, k in enumerate(columns):
                out[:, at * HD : (at + 1) * HD] = share[:, k * HD : (k + 1) * HD].astype(out.dtype)


def spread(hidden, index, grads, rows, sides, adds):
    seq_len = hidden.shape[0]
    n_z, n_dp, n_parts = index.shape[0] - 1, len(grads), len(sides)
    span = rows // n_parts
    width = n_dp * HD
    out_specs, out_shape = [], []
    for p in range(n_parts):
        for columns in sides[p]:
            wide = len(columns) * HD
            out_specs.append(pl.BlockSpec((span, wide), lambda i, at: (i, 0)))
            out_shape.append(jax.ShapeDtypeStruct((n_z * span, wide), jnp.bfloat16))
    outs = pl.pallas_call(
        functools.partial(spread_kernel, n_dp, n_parts, sides, bool(adds)),
        grid_spec=pltpu.PrefetchScalarGridSpec(
            num_scalar_prefetch=1,
            grid=(n_z,),
            in_specs=[pl.BlockSpec((seq_len, rows), lambda i, at: (0, at[i]))]
            + [pl.BlockSpec((seq_len, HD), lambda i, at: (0, 0))] * n_dp
            + [pl.BlockSpec((span, width), lambda i, at: (i, 0))] * len(adds),
            out_specs=out_specs,
            scratch_shapes=[pltpu.VMEM((seq_len, width), jnp.bfloat16)],
        ),
        out_shape=out_shape,
        cost_estimate=pl.CostEstimate(
            flops=8 * seq_len * n_z * rows * width,
            bytes_accessed=2 * n_z * rows * (seq_len + width),
            transcendentals=0,
        ),
        name="spread",
    )(index, hidden, *grads, *adds)
    per = len(sides[0])
    return [outs[p * per : (p + 1) * per] for p in range(n_parts)]


def after(value, *others):
    return lax.optimization_barrier((value, others))[0]


def attend_kernel(
    group, block, index_ref, keys_ref, values_ref, queries_ref, grads_ref, cos_ref, sin_ref, *rest
):
    context_ref, key_grad_ref, value_grad_ref, key_acc, value_acc = rest[-5:]
    del index_ref
    f32, bf16 = jnp.float32, jnp.bfloat16
    seq_len, head_dim = keys_ref.shape
    half = head_dim // 2
    factor = 1.0 / math.sqrt(head_dim)
    cosine, sine = cos_ref[...], sin_ref[...]
    raw = keys_ref[...].astype(f32)
    turned = jnp.concatenate([-raw[:, half:], raw[:, :half]], axis=1)
    keys = (raw * cosine + turned * sine).astype(bf16)
    values = values_ref[...]
    values_t = values.T
    outer = (((1,), (1,)), ((), ()))
    key_acc[...] = jnp.zeros_like(key_acc)
    value_acc[...] = jnp.zeros_like(value_acc)
    for j in range(seq_len // block):
        low, top = j * block, (j + 1) * block
        query = jnp.concatenate(
            [queries_ref[low:top, g * head_dim : (g + 1) * head_dim] for g in range(group)], axis=0
        )
        grad = jnp.concatenate(
            [grads_ref[low:top, g * head_dim : (g + 1) * head_dim] for g in range(group)], axis=0
        )
        scores = lax.dot_general(keys[:top], query, outer, preferred_element_type=f32)
        key_at = lax.broadcasted_iota(jnp.int32, scores.shape, 0)
        query_at = lax.broadcasted_iota(jnp.int32, scores.shape, 1) % block + low
        scores = jnp.where(key_at <= query_at, scores * factor, -1e30)
        weights = jnp.exp(scores - jnp.max(scores, axis=0, keepdims=True))
        probs = weights * (1.0 / jnp.sum(weights, axis=0, keepdims=True))
        probs_low = probs.astype(bf16)
        context = jnp.dot(values_t[:, :top], probs_low, preferred_element_type=f32).T.astype(bf16)
        for g in range(group):
            context_ref[low:top, g * head_dim : (g + 1) * head_dim] = context[
                g * block : (g + 1) * block
            ]
        value_acc[:top] += jnp.dot(probs_low, grad, preferred_element_type=f32)
        dprobs = lax.dot_general(values[:top], grad, outer, preferred_element_type=f32)
        inner = jnp.sum(dprobs * probs, axis=0, keepdims=True)
        dscores = (probs * (dprobs - inner) * factor).astype(bf16)
        key_acc[:top] += jnp.dot(dscores, query, preferred_element_type=f32)
    value_grad_ref[...] = value_acc[...].astype(bf16)
    rot = key_acc[...]
    scaled = rot * sine
    back = jnp.concatenate([scaled[:, half:], -scaled[:, :half]], axis=1)
    key_grad_ref[...] = (rot * cosine + back).astype(bf16)


def attend(kv, key_at, value_at, head, queries, cotangent, tables, context):
    seq_len = kv.shape[0]
    group = queries.shape[1] // (KVH * HD)
    wide = group * HD
    index = jnp.stack([key_at, value_at]).astype(jnp.int32)
    block = min(128, seq_len)
    whole = pl.BlockSpec((seq_len, HD), lambda i, at: (0, 0))
    in_specs = [
        pl.BlockSpec((seq_len, HD), lambda i, at: (0, at[0])),
        pl.BlockSpec((seq_len, HD), lambda i, at: (0, at[1])),
        pl.BlockSpec((seq_len, wide), lambda i, at: (0, head)),
        pl.BlockSpec((seq_len, wide), lambda i, at: (0, head)),
        whole,
        whole,
    ]
    operands = [index, kv, kv, queries, cotangent, *tables]
    aliases = {}
    if context is not None:
        in_specs.append(pl.BlockSpec(memory_space=pl.ANY))
        aliases = {len(operands): 0}
        operands.append(context)
    return pl.pallas_call(
        functools.partial(attend_kernel, group, block),
        grid_spec=pltpu.PrefetchScalarGridSpec(
            num_scalar_prefetch=1,
            grid=(1,),
            in_specs=in_specs,
            out_specs=[
                pl.BlockSpec((seq_len, wide), lambda i, at: (0, head)),
                whole,
                whole,
            ],
            scratch_shapes=[pltpu.VMEM((seq_len, HD), jnp.float32)] * 2,
        ),
        out_shape=[
            jax.ShapeDtypeStruct(queries.shape, jnp.bfloat16),
            jax.ShapeDtypeStruct((seq_len, HD), jnp.bfloat16),
            jax.ShapeDtypeStruct((seq_len, HD), jnp.bfloat16),
        ],
        input_output_aliases=aliases,
        cost_estimate=pl.CostEstimate(
            flops=10 * group * seq_len * seq_len * HD * 4,
            bytes_accessed=6 * seq_len * wide,
            transcendentals=group * seq_len * seq_len,
        ),
        name="attend",
    )(*operands)


def local(hidden, queries, cotangent, point_start, point_mid, point_end, curve_time):
    f32, bf16 = jnp.float32, jnp.bfloat16
    t_value = curve_time[0]
    bernstein = 2.0 * t_value * (1.0 - t_value)
    blended = (
        (1.0 - t_value) ** 2 * point_start.astype(f32)
        + bernstein * point_mid.astype(f32)
        + t_value**2 * point_end.astype(f32)
    ).astype(bf16)
    rows, columns = blended.shape
    n_dp, n_fsdp = lax.axis_size("dp"), lax.axis_size("fsdp")
    me_dp, me_fsdp = lax.axis_index("dp"), lax.axis_index("fsdp")
    chunks = columns // HD
    heads = KVH // chunks
    n_parts = 2 if (rows // 2) % 128 == 0 else 1
    span = rows // n_parts

    dp_masks = [1 << b for b in range(n_dp.bit_length() - 1)]
    dp_orders = [dp_masks, dp_masks[::-1]][:n_parts]
    n_z = n_fsdp // 2
    index = [
        jnp.stack([(2 * z + core) ^ me_fsdp for z in range(n_z)]).astype(jnp.int32)
        for core in (0, 1)
    ]
    index_dp = [jnp.append(i, me_dp.astype(jnp.int32)) for i in index]
    tables = rope_tables(hidden.shape[0], HD)

    def gather_outer(own):
        return [own] + [swap(own, 2 * z) for z in range(1, n_z)]

    def gather_dp(held, masks):
        pieces, arrays = {0: (held, 0)}, [held]
        for mask in masks:
            keys = sorted(pieces)
            if len(keys) > 1:
                sent = jnp.concatenate(
                    [pieces[k][0][:, pieces[k][1] * HD : (pieces[k][1] + 1) * HD] for k in keys],
                    axis=1,
                )
            else:
                sent = held
            got = swap(sent, mask * n_fsdp)
            arrays.append(got)
            for at, k in enumerate(keys):
                pieces[k ^ mask] = (got, at)
        return [pieces[k] for k in range(n_dp)], arrays

    gathered = []
    stages = []
    previous = None
    for c in range(chunks):
        own = blended[:, c * HD : (c + 1) * HD]
        if previous is not None:
            own = after(own, *previous)
        blocks = gather_outer(own)
        previous = blocks[1:]
        parts = []
        for p, masks in enumerate(dp_orders):
            held = jnp.concatenate([b[p * span : (p + 1) * span] for b in blocks], axis=0)
            if stages:
                held = after(held, *[a[-1] for a in stages[-1]])
            parts.append(gather_dp(held, masks))
        gathered.append([g[0] for g in parts])
        stages.append([g[1] for g in parts])

    def projected(c):
        parts = gathered[c]
        total = project(hidden, index[0], parts, rows, None, f32)
        other = []
        for part, arrays in zip(parts, stages[c]):
            swapped = [swap(a, 1) for a in arrays]
            names = [id(a) for a in arrays]
            other.append([(swapped[names.index(id(a))], at) for a, at in part])
        return project(hidden, index[1], other, rows, total, bf16)

    n_all = [list(range(n_dp))]
    splits = []
    for masks in dp_orders:
        last = masks[-1]
        stay = [k for k in range(n_dp) if not k & last]
        splits.append([stay, [k ^ last for k in stay]])

    projections = [projected(c) for c in range(chunks)]
    context = None
    ongoing = None
    sums = []

    def first_stage(halves):
        state = []
        for (stay, sent), masks, (columns, _) in zip(halves, dp_orders, splits):
            back = swap(sent, masks[-1] * n_fsdp)
            state.append(
                {
                    k: stay[:, at * HD : (at + 1) * HD].astype(f32)
                    + back[:, at * HD : (at + 1) * HD].astype(f32)
                    for at, k in enumerate(columns)
                }
            )
        return state

    def later_stages(state):
        done = []
        for pieces, masks in zip(state, dp_orders):
            for mask in reversed(masks[:-1]):
                stay = [k for k in sorted(pieces) if not k & mask]
                sent = jnp.concatenate([pieces[k ^ mask].astype(bf16) for k in stay], axis=1)
                back = swap(sent, mask * n_fsdp)
                pieces = {
                    k: pieces[k] + back[:, at * HD : (at + 1) * HD].astype(f32)
                    for at, k in enumerate(stay)
                }
            done.append(pieces[0])
        return done

    def last_stage(done):
        out = []
        for held in done:
            low = held.astype(bf16)
            total = held[:span]
            for z in range(1, n_z):
                total = total + swap(low[z * span : (z + 1) * span], 2 * z).astype(f32)
            out.append(total)
        return jnp.concatenate(out, axis=0)

    for c in range(chunks):
        grads = {}
        for i in range(heads):
            kv = projections[c]
            if c + 1 < chunks and i == heads - 1:
                kv = after(kv, *[a[1] for a in stages[c + 1]])
            context, key_grad, value_grad = attend(
                kv,
                i ^ me_dp,
                (i + heads) ^ me_dp,
                i * chunks + c,
                queries,
                cotangent,
                tables,
                context,
            )
            grads[i], grads[i + heads] = key_grad, value_grad
        blocks = [grads[k] for k in range(n_dp)]
        if c + 1 < chunks:
            blocks[0] = after(blocks[0], *[a[-1] for a in stages[c + 1]])
        if ongoing is not None:
            blocks[0], ongoing = lax.optimization_barrier((blocks[0], ongoing))
        sent = spread(hidden, index_dp[1], blocks, rows, [n_all] * n_parts, [])
        got = [swap(s[0], 1) for s in sent]
        if ongoing is not None:
            ongoing = later_stages(ongoing)
            got, ongoing = lax.optimization_barrier((got, ongoing))
        halves = spread(hidden, index_dp[0], blocks, rows, splits, got)
        if c + 1 < chunks:
            halves, projections[c + 1] = lax.optimization_barrier((halves, projections[c + 1]))
        if ongoing is not None:
            sums.append(last_stage(ongoing))
        ongoing = first_stage(halves)
    sums.append(last_stage(later_stages(ongoing)))
    gradient = jnp.concatenate(sums, axis=1) * bernstein
    return (context, gradient)


def solution(mesh):
    return jax.shard_map(
        local,
        mesh=mesh,
        in_specs=(
            P(AXES, None),
            P(AXES, None),
            P(AXES, None),
            P("fsdp", "dp"),
            P("fsdp", "dp"),
            P("fsdp", "dp"),
            P(),
        ),
        out_specs=(P(AXES, None), P("fsdp", "dp")),
        check_vma=False,
    )
```

```python
import functools
import math

import jax
import jax.numpy as jnp
from jax import lax
from jax.experimental import pallas as pl
from jax.experimental.pallas import tpu as pltpu
from jax.sharding import PartitionSpec as P

KVH = 4
HD = 128
AXES = ("dp", "fsdp")


def rope_tables(seq_len, head_dim):
    positions = jnp.arange(seq_len, dtype=jnp.float32)[:, None]
    halves_index = jnp.arange(head_dim // 2, dtype=jnp.float32)[None, :]
    inverse = jnp.exp(-(2.0 * halves_index / head_dim) * math.log(500000.0))
    angles = positions * inverse
    cosine = jnp.concatenate([jnp.cos(angles), jnp.cos(angles)], axis=1)
    sine_t = jnp.concatenate([jnp.sin(angles), jnp.sin(angles)], axis=1)
    return (cosine, sine_t)


def swap(value, mask):
    count = lax.axis_size("dp") * lax.axis_size("fsdp")
    return lax.ppermute(value, AXES, [(i, i ^ mask) for i in range(count)])


def project_kernel(layout, has_sum, index_ref, hidden_ref, *rest):
    del index_ref
    refs, sum_ref, out_ref, acc_ref = rest[:-3], rest[-3], rest[-2], rest[-1]
    step = pl.program_id(0)
    blocks = []
    for part in layout:
        blocks.append(jnp.concatenate([refs[at][...] for at in part], axis=1))
    product = jnp.dot(
        hidden_ref[...], jnp.concatenate(blocks, axis=0), preferred_element_type=jnp.float32
    )

    @pl.when(step == 0)
    def _():
        acc_ref[...] = product + sum_ref[...] if has_sum else product

    @pl.when(step > 0)
    def _():
        acc_ref[...] += product

    @pl.when(step == pl.num_programs(0) - 1)
    def _():
        out_ref[...] = acc_ref[...].astype(out_ref.dtype)


def project(hidden, index, parts, rows, total, dtype):
    seq_len = hidden.shape[0]
    n_z = index.shape[0]
    span = rows // len(parts)
    flat, layout = [], []
    for part in parts:
        layout.append(list(range(len(flat), len(flat) + len(part))))
        flat.extend(part)
    width = HD * len(parts[0])
    whole = pl.BlockSpec((seq_len, width), lambda i, at: (0, 0))
    has_sum = total is not None
    if total is None:
        total = jnp.zeros((8, HD), jnp.float32)
    sum_spec = whole if has_sum else pl.BlockSpec((8, HD), lambda i, at: (0, 0))
    specs = [pl.BlockSpec((span, HD), lambda i, at, c=c: (i, c)) for _, c in flat]
    return pl.pallas_call(
        functools.partial(project_kernel, layout, has_sum),
        grid_spec=pltpu.PrefetchScalarGridSpec(
            num_scalar_prefetch=1,
            grid=(n_z,),
            in_specs=[pl.BlockSpec((seq_len, rows), lambda i, at: (0, at[i]))] + specs + [sum_spec],
            out_specs=whole,
            scratch_shapes=[pltpu.VMEM((seq_len, width), jnp.float32)],
        ),
        out_shape=jax.ShapeDtypeStruct((seq_len, width), dtype),
        cost_estimate=pl.CostEstimate(
            flops=8 * seq_len * n_z * rows * width,
            bytes_accessed=2 * n_z * rows * (seq_len + width),
            transcendentals=0,
        ),
        name="project",
    )(index, hidden, *[array for array, _ in flat], total)


def spread_kernel(n_dp, n_parts, sides, has_add, index_ref, hidden_ref, *rest):
    grads, rest = rest[:n_dp], rest[n_dp:]
    adds, outs, relative_ref = rest[: len(rest) - 1 - n_parts * len(sides[0])], None, rest[-1]
    outs = rest[len(adds) : -1]
    step = pl.program_id(0)

    @pl.when(step == 0)
    def _():
        me = index_ref[index_ref.shape[0] - 1]
        for k in range(n_dp):
            to = pl.multiple_of((k ^ me) * HD, HD)
            relative_ref[:, pl.ds(to, HD)] = grads[k][...]

    product = lax.dot_general(
        hidden_ref[...],
        relative_ref[...],
        (((0,), (0,)), ((), ())),
        preferred_element_type=jnp.float32,
    )
    span = product.shape[0] // n_parts
    for p in range(n_parts):
        share = product[p * span : (p + 1) * span]
        if has_add:
            share = share + adds[p][...].astype(jnp.float32)
        for side, columns in enumerate(sides[p]):
            out = outs[p * len(sides[p]) + side]
            for at, k in enumerate(columns):
                out[:, at * HD : (at + 1) * HD] = share[:, k * HD : (k + 1) * HD].astype(out.dtype)


def spread(hidden, index, grads, rows, sides, adds):
    seq_len = hidden.shape[0]
    n_z, n_dp, n_parts = index.shape[0] - 1, len(grads), len(sides)
    span = rows // n_parts
    width = n_dp * HD
    out_specs, out_shape = [], []
    for p in range(n_parts):
        for columns in sides[p]:
            wide = len(columns) * HD
            out_specs.append(pl.BlockSpec((span, wide), lambda i, at: (i, 0)))
            out_shape.append(jax.ShapeDtypeStruct((n_z * span, wide), jnp.bfloat16))
    outs = pl.pallas_call(
        functools.partial(spread_kernel, n_dp, n_parts, sides, bool(adds)),
        grid_spec=pltpu.PrefetchScalarGridSpec(
            num_scalar_prefetch=1,
            grid=(n_z,),
            in_specs=[pl.BlockSpec((seq_len, rows), lambda i, at: (0, at[i]))]
            + [pl.BlockSpec((seq_len, HD), lambda i, at: (0, 0))] * n_dp
            + [pl.BlockSpec((span, width), lambda i, at: (i, 0))] * len(adds),
            out_specs=out_specs,
            scratch_shapes=[pltpu.VMEM((seq_len, width), jnp.bfloat16)],
        ),
        out_shape=out_shape,
        cost_estimate=pl.CostEstimate(
            flops=8 * seq_len * n_z * rows * width,
            bytes_accessed=2 * n_z * rows * (seq_len + width),
            transcendentals=0,
        ),
        name="spread",
    )(index, hidden, *grads, *adds)
    per = len(sides[0])
    return [outs[p * per : (p + 1) * per] for p in range(n_parts)]


def after(value, *others):
    return lax.optimization_barrier((value, others))[0]


def attend_kernel(
    group, block, index_ref, keys_ref, values_ref, queries_ref, grads_ref, cos_ref, sin_ref, *rest
):
    context_ref, key_grad_ref, value_grad_ref, key_acc, value_acc = rest[-5:]
    del index_ref
    f32, bf16 = jnp.float32, jnp.bfloat16
    seq_len, head_dim = keys_ref.shape
    half = head_dim // 2
    factor = 1.0 / math.sqrt(head_dim)
    cosine, sine = cos_ref[...], sin_ref[...]
    raw = keys_ref[...].astype(f32)
    turned = jnp.concatenate([-raw[:, half:], raw[:, :half]], axis=1)
    keys = (raw * cosine + turned * sine).astype(bf16)
    values = values_ref[...]
    values_t = values.T
    outer = (((1,), (1,)), ((), ()))
    key_acc[...] = jnp.zeros_like(key_acc)
    value_acc[...] = jnp.zeros_like(value_acc)
    for j in range(seq_len // block):
        low, top = j * block, (j + 1) * block
        query = jnp.concatenate(
            [queries_ref[low:top, g * head_dim : (g + 1) * head_dim] for g in range(group)], axis=0
        )
        grad = jnp.concatenate(
            [grads_ref[low:top, g * head_dim : (g + 1) * head_dim] for g in range(group)], axis=0
        )
        scores = lax.dot_general(keys[:top], query, outer, preferred_element_type=f32)
        key_at = lax.broadcasted_iota(jnp.int32, scores.shape, 0)
        query_at = lax.broadcasted_iota(jnp.int32, scores.shape, 1) % block + low
        scores = jnp.where(key_at <= query_at, scores * factor, -1e30)
        weights = jnp.exp(scores - jnp.max(scores, axis=0, keepdims=True))
        probs = weights * (1.0 / jnp.sum(weights, axis=0, keepdims=True))
        probs_low = probs.astype(bf16)
        context = jnp.dot(values_t[:, :top], probs_low, preferred_element_type=f32).T.astype(bf16)
        for g in range(group):
            context_ref[low:top, g * head_dim : (g + 1) * head_dim] = context[
                g * block : (g + 1) * block
            ]
        value_acc[:top] += jnp.dot(probs_low, grad, preferred_element_type=f32)
        dprobs = lax.dot_general(values[:top], grad, outer, preferred_element_type=f32)
        inner = jnp.sum(dprobs * probs, axis=0, keepdims=True)
        dscores = (probs * (dprobs - inner) * factor).astype(bf16)
        key_acc[:top] += jnp.dot(dscores, query, preferred_element_type=f32)
    value_grad_ref[...] = value_acc[...].astype(bf16)
    rot = key_acc[...]
    scaled = rot * sine
    back = jnp.concatenate([scaled[:, half:], -scaled[:, :half]], axis=1)
    key_grad_ref[...] = (rot * cosine + back).astype(bf16)


def attend(kv, key_at, value_at, head, queries, cotangent, tables, context):
    seq_len = kv.shape[0]
    group = queries.shape[1] // (KVH * HD)
    wide = group * HD
    index = jnp.stack([key_at, value_at]).astype(jnp.int32)
    block = min(128, seq_len)
    whole = pl.BlockSpec((seq_len, HD), lambda i, at: (0, 0))
    in_specs = [
        pl.BlockSpec((seq_len, HD), lambda i, at: (0, at[0])),
        pl.BlockSpec((seq_len, HD), lambda i, at: (0, at[1])),
        pl.BlockSpec((seq_len, wide), lambda i, at: (0, head)),
        pl.BlockSpec((seq_len, wide), lambda i, at: (0, head)),
        whole,
        whole,
    ]
    operands = [index, kv, kv, queries, cotangent, *tables]
    aliases = {}
    if context is not None:
        in_specs.append(pl.BlockSpec(memory_space=pl.ANY))
        aliases = {len(operands): 0}
        operands.append(context)
    return pl.pallas_call(
        functools.partial(attend_kernel, group, block),
        grid_spec=pltpu.PrefetchScalarGridSpec(
            num_scalar_prefetch=1,
            grid=(1,),
            in_specs=in_specs,
            out_specs=[
                pl.BlockSpec((seq_len, wide), lambda i, at: (0, head)),
                whole,
                whole,
            ],
            scratch_shapes=[pltpu.VMEM((seq_len, HD), jnp.float32)] * 2,
        ),
        out_shape=[
            jax.ShapeDtypeStruct(queries.shape, jnp.bfloat16),
            jax.ShapeDtypeStruct((seq_len, HD), jnp.bfloat16),
            jax.ShapeDtypeStruct((seq_len, HD), jnp.bfloat16),
        ],
        input_output_aliases=aliases,
        cost_estimate=pl.CostEstimate(
            flops=10 * group * seq_len * seq_len * HD * 4,
            bytes_accessed=6 * seq_len * wide,
            transcendentals=group * seq_len * seq_len,
        ),
        name="attend",
    )(*operands)


def local(hidden, queries, cotangent, point_start, point_mid, point_end, curve_time):
    f32, bf16 = jnp.float32, jnp.bfloat16
    t_value = curve_time[0]
    bernstein = 2.0 * t_value * (1.0 - t_value)
    blended = (
        (1.0 - t_value) ** 2 * point_start.astype(f32)
        + bernstein * point_mid.astype(f32)
        + t_value**2 * point_end.astype(f32)
    ).astype(bf16)
    rows, columns = blended.shape
    n_dp, n_fsdp = lax.axis_size("dp"), lax.axis_size("fsdp")
    me_dp, me_fsdp = lax.axis_index("dp"), lax.axis_index("fsdp")
    chunks = columns // HD
    heads = KVH // chunks
    n_parts = 2 if (rows // 2) % 128 == 0 else 1
    span = rows // n_parts

    dp_masks = [1 << b for b in range(n_dp.bit_length() - 1)]
    dp_orders = [dp_masks, dp_masks[::-1]][:n_parts]
    n_z = n_fsdp // 2
    index = [
        jnp.stack([(2 * z + core) ^ me_fsdp for z in range(n_z)]).astype(jnp.int32)
        for core in (0, 1)
    ]
    index_dp = [jnp.append(i, me_dp.astype(jnp.int32)) for i in index]
    tables = rope_tables(hidden.shape[0], HD)

    def gather_outer(own):
        return [own] + [swap(own, 2 * z) for z in range(1, n_z)]

    def gather_dp(held, masks):
        pieces, arrays = {0: (held, 0)}, [held]
        for mask in masks:
            keys = sorted(pieces)
            if len(keys) > 1:
                sent = jnp.concatenate(
                    [pieces[k][0][:, pieces[k][1] * HD : (pieces[k][1] + 1) * HD] for k in keys],
                    axis=1,
                )
            else:
                sent = held
            got = swap(sent, mask * n_fsdp)
            arrays.append(got)
            for at, k in enumerate(keys):
                pieces[k ^ mask] = (got, at)
        return [pieces[k] for k in range(n_dp)], arrays

    gathered = []
    stages = []
    previous = None
    for c in range(chunks):
        own = blended[:, c * HD : (c + 1) * HD]
        if previous is not None:
            own = after(own, *previous)
        blocks = gather_outer(own)
        parts = []
        for p, masks in enumerate(dp_orders):
            held = jnp.concatenate([b[p * span : (p + 1) * span] for b in blocks], axis=0)
            if stages:
                held = after(held, *[a[-1] for a in stages[-1]])
            parts.append(gather_dp(held, masks))
        gathered.append([g[0] for g in parts])
        stages.append([g[1] for g in parts])
        previous = [a[1] for a in stages[-1]]

    def projected(c):
        parts = gathered[c]
        total = project(hidden, index[0], parts, rows, None, f32)
        other = []
        for part, arrays in zip(parts, stages[c]):
            swapped = [swap(a, 1) for a in arrays]
            names = [id(a) for a in arrays]
            other.append([(swapped[names.index(id(a))], at) for a, at in part])
        return project(hidden, index[1], other, rows, total, bf16)

    n_all = [list(range(n_dp))]
    splits = []
    for masks in dp_orders:
        last = masks[-1]
        stay = [k for k in range(n_dp) if not k & last]
        splits.append([stay, [k ^ last for k in stay]])

    projections = [projected(c) for c in range(chunks)]
    context = None
    ongoing = None
    sums = []

    def first_stage(halves):
        state = []
        for (stay, sent), masks, (columns, _) in zip(halves, dp_orders, splits):
            back = swap(sent, masks[-1] * n_fsdp)
            state.append(
                {
                    k: stay[:, at * HD : (at + 1) * HD].astype(f32)
                    + back[:, at * HD : (at + 1) * HD].astype(f32)
                    for at, k in enumerate(columns)
                }
            )
        return state

    def later_stages(state):
        done = []
        for pieces, masks in zip(state, dp_orders):
            for mask in reversed(masks[:-1]):
                stay = [k for k in sorted(pieces) if not k & mask]
                sent = jnp.concatenate([pieces[k ^ mask].astype(bf16) for k in stay], axis=1)
                back = swap(sent, mask * n_fsdp)
                pieces = {
                    k: pieces[k] + back[:, at * HD : (at + 1) * HD].astype(f32)
                    for at, k in enumerate(stay)
                }
            done.append(pieces[0])
        return done

    def last_stage(done):
        out = []
        for held in done:
            low = held.astype(bf16)
            total = held[:span]
            for z in range(1, n_z):
                total = total + swap(low[z * span : (z + 1) * span], 2 * z).astype(f32)
            out.append(total)
        return jnp.concatenate(out, axis=0)

    for c in range(chunks):
        grads = {}
        for i in range(heads):
            kv = projections[c]
            if c + 1 < chunks and i == heads - 1:
                kv = after(kv, *[a[1] for a in stages[c + 1]])
            context, key_grad, value_grad = attend(
                kv,
                i ^ me_dp,
                (i + heads) ^ me_dp,
                i * chunks + c,
                queries,
                cotangent,
                tables,
                context,
            )
            grads[i], grads[i + heads] = key_grad, value_grad
        blocks = [grads[k] for k in range(n_dp)]
        if c + 1 < chunks:
            blocks[0] = after(blocks[0], *[a[-1] for a in stages[c + 1]])
        if ongoing is not None:
            blocks[0], ongoing = lax.optimization_barrier((blocks[0], ongoing))
        sent = spread(hidden, index_dp[1], blocks, rows, [n_all] * n_parts, [])
        got = [swap(s[0], 1) for s in sent]
        if ongoing is not None:
            ongoing = later_stages(ongoing)
            got, ongoing = lax.optimization_barrier((got, ongoing))
        halves = spread(hidden, index_dp[0], blocks, rows, splits, got)
        if c + 1 < chunks:
            halves, projections[c + 1] = lax.optimization_barrier((halves, projections[c + 1]))
        if ongoing is not None:
            sums.append(last_stage(ongoing))
        ongoing = first_stage(halves)
    sums.append(last_stage(later_stages(ongoing)))
    gradient = jnp.concatenate(sums, axis=1) * bernstein
    return (context, gradient)


def solution(mesh):
    return jax.shard_map(
        local,
        mesh=mesh,
        in_specs=(
            P(AXES, None),
            P(AXES, None),
            P(AXES, None),
            P("fsdp", "dp"),
            P("fsdp", "dp"),
            P("fsdp", "dp"),
            P(),
        ),
        out_specs=(P(AXES, None), P("fsdp", "dp")),
        check_vma=False,
    )
```
